256 devices in a mesh: row: 32 (over x, y, core), col: 8 (over z).
Axes of the slice: x: 4, y: 4, z: 8, core: 2. Of those that a mesh axis runs over, the one named last changes fastest.
Arguments:
- matrix: float32 [5120, 5120], P('row', 'col'), may hold values from -64 to 64
Outputs:
- iterate: float32 [5120, 5120], P('row', 'col')
- trace_value: float32 [2], replicated
- frobenius: float32 [2], replicated
The draws below stay inside these ranges and needn't reach their ends.
All inputs are finite; a program needn't handle non-finite values.
Results may differ from the reference program's by a relative error of at most 0.003.
Values may be sent and summed in bfloat16 or wider, within the bound.
No kernel may reach another device: no remote copies, remote signals or barrier semaphores. Data moves between devices by JAX's collectives and lax.ppermute only.
A program may use at most 64 MiB of HBM per device.

```python
import math
import jax
import jax.numpy as jnp

ORDER = 5120


def draw_matrix(key, part):
    first, second, third = jax.random.split(key, 3)
    ramp = jnp.arange(ORDER, dtype=jnp.float32) / max(ORDER - 1, 1)
    raw = jax.random.truncated_normal(first, -5.0, 5.0, (ORDER, ORDER), jnp.float32)
    base = jnp.exp(jax.random.uniform(second, (ORDER,), jnp.float32, math.log(0.6), math.log(1.9)))
    shift = jax.random.uniform(third, (ORDER,), jnp.float32, -0.5, 1.5)
    scales = base * (1.0 + 0.7 * ramp)
    wigner = (raw + raw.T) / jnp.sqrt(2.0 * ORDER)
    inner = wigner + jnp.diag(shift)
    return scales[:, None] * inner * scales[None, :]


def setup_inputs(seed: int = 0) -> dict:
    splits = jax.random.split(jax.random.key(seed), 2)
    matrix = draw_matrix(jax.random.fold_in(splits[1], 71), 0)
    return dict(matrix=matrix)


target = 0.0625

def sign_step(current, rounded, scale, root):
    product = jnp.dot(rounded, rounded, preferred_element_type=jnp.float32)
    squared = (product * scale).astype(jnp.bfloat16)
    cubic_part = jnp.dot(squared, rounded, preferred_element_type=jnp.float32)
    return root * (1.5 * current - 0.5 * cubic_part)

def reference(matrix):
    rounded = matrix.astype(jnp.bfloat16)
    widened = rounded.astype(jnp.float32)
    squares = jnp.sum(widened * widened)
    factor = target * ORDER / (squares + 1e-06)
    first = sign_step(widened, rounded, factor, jnp.sqrt(factor))
    second = sign_step(first, first.astype(jnp.bfloat16), jnp.float32(1.0), jnp.float32(1.0))
    traces = jnp.stack([jnp.sum(jnp.diagonal(first)), jnp.sum(jnp.diagonal(second))])
    norms = jnp.stack([jnp.sqrt(jnp.sum(first * first)), jnp.sqrt(jnp.sum(second * second))])
    return (second, traces, norms)
```

```python
import functools
import jax
import jax.numpy as jnp
import numpy as np
from jax import lax
from jax.experimental import pallas as pl
from jax.experimental.pallas import tpu as pltpu
from jax.sharding import Mesh
from jax.sharding import PartitionSpec as P

NX, NY, NC, NZ = 4, 4, 2, 8
AXES = ("x", "y", "c", "z")
TARGET = 0.0625

EVERY = [
    (x, y, c, z) for x in range(NX) for y in range(NY) for c in range(NC) for z in range(NZ)
]


def rank(x, y, c, z):
    return ((x * NY + y) * NC + c) * NZ + z


def even_pair(i, n):
    return i ^ 1


def odd_pair(i, n):
    return (((i - 1) % n ^ 1) + 1) % n


PAIRS = (even_pair, odd_pair)


def permute(value, target):
    return lax.ppermute(value, AXES, [(rank(*d), rank(*target(*d))) for d in EVERY])


def along_z(turn):
    return lambda x, y, c, z: (x, y, c, PAIRS[turn ^ c](z, NZ))


def along_xy(second, turn):
    def target(x, y, c, z):
        if second ^ c:
            return (x, PAIRS[turn](y, NY), c, z)
        return (PAIRS[turn](x, NX), y, c, z)

    return target


def sibling(value):
    return permute(value, lambda x, y, c, z: (x, y, 1 - c, z))


def join(*parts):
    return jnp.concatenate(parts, axis=0)


def z_order(c, z):
    a, b = PAIRS[c], PAIRS[1 - c]
    two = lambda i: [i, a(i, NZ)]
    third = b(a(z, NZ), NZ)
    fourth = b(a(b(z, NZ), NZ), NZ)
    return two(z) + two(b(z, NZ)) + two(third) + two(fourth)


def xy_order(x, y, c):
    places = []
    for core in (c, 1 - c):
        for half in range(2):
            a, b = PAIRS[half], PAIRS[1 - half]
            i, j = (x, y) if core == 0 else (y, x)
            four = lambda k: [k, a(k, 4), b(k, 4), a(b(k, 4), 4)]
            for jj in four(j):
                for ii in four(i):
                    xx, yy = (ii, jj) if core == 0 else (jj, ii)
                    places.append(((xx * NY + yy) * NC + core) * 2 + half)
    return places


def order_table():
    return np.array(
        [xy_order(x, y, c) + z_order(c, z) for (x, y, c, z) in EVERY], dtype=np.int32
    )


def vmem():
    return pl.BlockSpec(memory_space=pltpu.VMEM)


def smem():
    return pl.BlockSpec(memory_space=pltpu.SMEM)


def fold(values):
    rows, cols = values.shape
    total = jnp.zeros((8, 128), jnp.float32)
    for r in range(0, rows, 8):
        for k in range(0, cols, 128):
            total = total + values[r : r + 8, k : k + 128]
    return total


def prepare_body(matrix, tile, top, bottom):
    half = tile.shape[0] // 2
    rounded = matrix[...].astype(jnp.bfloat16)
    tile[...] = rounded
    top[...] = rounded[:half]
    bottom[...] = rounded[half:]


def prepare(matrix):
    rows, cols = matrix.shape
    shapes = [(rows, cols), (rows // 2, cols), (rows // 2, cols)]
    return pl.pallas_call(
        prepare_body,
        out_shape=[jax.ShapeDtypeStruct(s, jnp.bfloat16) for s in shapes],
        in_specs=[vmem()],
        out_specs=[vmem()] * 3,
        name="prepare",
    )(matrix)


def lay_rows(order, base, pieces, wide, rows, cols):
    spot = base
    for piece in pieces:
        for k in range(piece.shape[0] // rows):
            start = pl.multiple_of(order[spot] * cols, 128)
            wide[:, pl.ds(start, cols)] = piece[k * rows : (k + 1) * rows, :]
            spot += 1


def multiply(wide, panel, total):
    block = 2 * total.shape[1]

    def add(k, carry):
        start = pl.multiple_of(k * block, block)
        part = jnp.dot(
            wide[:, pl.ds(start, block)],
            panel[pl.ds(start, block), :],
            preferred_element_type=jnp.float32,
        )
        total[...] += part
        return carry

    total[...] = jnp.zeros(total.shape, jnp.float32)
    lax.fori_loop(0, wide.shape[1] // block, add, 0)


def first_body(with_squares, n_right, n_left, order, *refs):
    right = refs[:n_right]
    left = refs[n_right : n_right + n_left]
    outs = refs[n_right + n_left :]
    out, panel = outs[0], outs[1]
    wide, summed = outs[-2], outs[-1]
    rows, cols = out.shape
    half = rows // 2
    spot = 0
    for piece in right:
        for k in range(piece.shape[0] // half):
            start = pl.multiple_of(order[spot] * half, half)
            panel[pl.ds(start, half), :] = piece[k * half : (k + 1) * half, :]
            spot += 1
    lay_rows(order, spot, left, wide, rows, cols)
    if with_squares:
        total = jnp.zeros((8, 128), jnp.float32)
        for k in range(wide.shape[1] // cols):
            part = wide[:, k * cols : (k + 1) * cols].astype(jnp.float32)
            total = total + fold(part * part)
        outs[2][...] = total
    multiply(wide, panel, summed)
    out[...] = summed[...].astype(jnp.bfloat16)


def first_product(order, right, left, rows, cols, with_squares):
    full = cols * NZ
    shapes = [
        jax.ShapeDtypeStruct((rows, cols), jnp.bfloat16),
        jax.ShapeDtypeStruct((full, cols), jnp.bfloat16),
    ]
    if with_squares:
        shapes.append(jax.ShapeDtypeStruct((8, 128), jnp.float32))
    return pl.pallas_call(
        functools.partial(first_body, with_squares, len(right), len(left)),
        out_shape=shapes,
        in_specs=[smem()] + [vmem()] * (len(right) + len(left)),
        out_specs=[vmem()] * len(shapes),
        scratch_shapes=[
            pltpu.VMEM((rows, full), jnp.bfloat16),
            pltpu.VMEM((rows, cols), jnp.float32),
        ],
        name="first_product",
        cost_estimate=pl.CostEstimate(
            flops=2 * rows * cols * full, bytes_accessed=2 * full * cols, transcendentals=0
        ),
    )(order, *right, *left)


def second_body(last, n_left, base, order, shift, scales, panel, current, *refs):
    left = refs[:n_left]
    outs = refs[n_left:]
    wide, summed = outs[-2], outs[-1]
    rows, cols = current.shape
    lay_rows(order, base, left, wide, rows, cols)
    multiply(wide, panel, summed)
    value = 1.5 * current[...].astype(jnp.float32) - 0.5 * (scales[0] * summed[...])
    value = scales[1] * value
    outs[0][...] = value
    r = lax.broadcasted_iota(jnp.int32, (rows, cols), 0)
    k = lax.broadcasted_iota(jnp.int32, (rows, cols), 1)
    stats = outs[1]
    stats[0] = fold(jnp.where(k - r == shift[0], value, 0.0))
    stats[1] = fold(value * value)
    if not last:
        rounded = value.astype(jnp.bfloat16)
        outs[2][...] = rounded
        outs[3][...] = rounded[: rows // 2]
        outs[4][...] = rounded[rows // 2 :]


def second_product(order, shift, scales, panel, current, left, last):
    rows, cols = current.shape
    full = cols * NZ
    shapes = [
        jax.ShapeDtypeStruct((rows, cols), jnp.float32),
        jax.ShapeDtypeStruct((2, 8, 128), jnp.float32),
    ]
    if not last:
        shapes.append(jax.ShapeDtypeStruct((rows, cols), jnp.bfloat16))
        shapes += [jax.ShapeDtypeStruct((rows // 2, cols), jnp.bfloat16)] * 2
    return pl.pallas_call(
        functools.partial(second_body, last, len(left), order.shape[0] - NZ),
        out_shape=shapes,
        in_specs=[smem()] * 3 + [vmem()] * (2 + len(left)),
        out_specs=[vmem()] * len(shapes),
        scratch_shapes=[
            pltpu.VMEM((rows, full), jnp.bfloat16),
            pltpu.VMEM((rows, cols), jnp.float32),
        ],
        name="second_product",
        cost_estimate=pl.CostEstimate(
            flops=2 * rows * cols * full, bytes_accessed=2 * full * cols, transcendentals=0
        ),
    )(order, shift, scales, panel, current, *left)


def in_step(*values):
    return lax.optimization_barrier(values)


def panels(tile, top, bottom):
    a, b, s = in_step(
        join(top, permute(top, along_xy(0, 0))),
        join(bottom, permute(bottom, along_xy(0, 1))),
        join(tile, permute(tile, along_z(0))),
    )
    left = [s]
    a, b, s = in_step(
        join(a, permute(a, along_xy(0, 1))),
        join(b, permute(b, along_xy(0, 0))),
        permute(s, along_z(1)),
    )
    left.append(s)
    a, b, s = in_step(
        join(a, permute(a, along_xy(1, 0))),
        join(b, permute(b, along_xy(1, 1))),
        permute(s, along_z(0)),
    )
    left.append(s)
    a4 = permute(a, along_xy(1, 1))
    b4 = permute(b, along_xy(1, 0))
    left.append(permute(s, along_z(1)))
    right = [a, a4, b, b4]
    return right + [sibling(v) for v in right], left


def row_panel(tile):
    two = join(tile, permute(tile, along_z(0)))
    second = permute(two, along_z(1))
    third = permute(second, along_z(0))
    return [two, second, third, permute(third, along_z(1))]


def add_over_rows(value):
    value = value + sibling(value)
    for second in range(2):
        for turn in range(2):
            value = value + permute(
                value,
                lambda x, y, c, z: (x, PAIRS[turn](y, NY), c, z)
                if second
                else (PAIRS[turn](x, NX), y, c, z),
            )
    return value


def add_over_z(value):
    for step in (1, 2, 4):
        value = value + permute(value, lambda x, y, c, z: (x, y, c, z ^ step))
    return value


def on_device(matrix):
    rows, cols = matrix.shape
    me = lax.axis_index(AXES)
    order = lax.dynamic_index_in_dim(jnp.asarray(order_table()), me, 0, keepdims=False)
    row_first = lax.axis_index(("x", "y", "c")) * rows
    shift = (row_first - lax.axis_index("z") * cols).reshape(1)
    tile, top, bottom = prepare(matrix)

    right, left = panels(tile, top, bottom)
    squared, panel, partial = first_product(order, right, left, rows, cols, True)
    squares = jnp.sum(add_over_rows(partial))
    scale = TARGET * (cols * NZ) / (squares + 1e-06)
    scales = jnp.stack([scale, jnp.sqrt(scale)])
    current, stats_first, tile, top, bottom = second_product(
        order, shift, scales, panel, tile, row_panel(squared), False
    )

    right, left = panels(tile, top, bottom)
    squared, panel = first_product(order, right, left, rows, cols, False)
    current, stats_second = second_product(
        order, shift, jnp.ones((2,), jnp.float32), panel, current, row_panel(squared), True
    )
    stats = jnp.stack([stats_first, stats_second]).reshape(32, 128)
    stats = add_over_z(add_over_rows(stats))
    sums = jnp.sum(stats.reshape(2, 2, 8, 128), axis=(2, 3))
    return (current, sums[:, 0], jnp.sqrt(sums[:, 1]))


def solution(mesh):
    split = Mesh(mesh.devices.reshape(NX, NY, NC, NZ), AXES)
    return jax.shard_map(
        on_device,
        mesh=split,
        in_specs=(P(("x", "y", "c"), "z"),),
        out_specs=(P(("x", "y", "c"), "z"), P(), P()),
        check_vma=False,
    )
```

```python
import functools
import jax
import jax.numpy as jnp
import numpy as np
from jax import lax
from jax.experimental import pallas as pl
from jax.experimental.pallas import tpu as pltpu
from jax.sharding import Mesh
from jax.sharding import PartitionSpec as P

NX, NY, NC, NZ = 4, 4, 2, 8
AXES = ("x", "y", "c", "z")
TARGET = 0.0625

EVERY = [
    (x, y, c, z) for x in range(NX) for y in range(NY) for c in range(NC) for z in range(NZ)
]


def rank(x, y, c, z):
    return ((x * NY + y) * NC + c) * NZ + z


def even_pair(i, n):
    return i ^ 1


def odd_pair(i, n):
    return (((i - 1) % n ^ 1) + 1) % n


PAIRS = (even_pair, odd_pair)


def permute(value, target):
    return lax.ppermute(value, AXES, [(rank(*d), rank(*target(*d))) for d in EVERY])


def along_z(turn):
    return lambda x, y, c, z: (x, y, 1 - c, PAIRS[turn ^ c ^ (z & 1)](z, NZ))


def along_xy(second, turn):
    def target(x, y, c, z):
        if second ^ c ^ ((x + y) & 1):
            return (x, PAIRS[turn](y, NY), 1 - c, z)
        return (PAIRS[turn](x, NX), y, 1 - c, z)

    return target


def join(*parts):
    return jnp.concatenate(parts, axis=0)


def z_order(group, z):
    a, b = PAIRS[group], PAIRS[1 - group]
    two = lambda i: [i, a(i, NZ)]
    third = b(a(z, NZ), NZ)
    fourth = b(a(b(z, NZ), NZ), NZ)
    return two(z) + two(b(z, NZ)) + two(third) + two(fourth)


def xy_places(x, y, group, half, flip):
    a, b = PAIRS[half], PAIRS[1 - half]
    i, j = (x, y) if group == 0 else (y, x)
    four = lambda k: [k, a(k, 4), b(k, 4), a(b(k, 4), 4)]
    places = []
    for jj in four(j):
        for ii in four(i):
            xx, yy = (ii, jj) if group == 0 else (jj, ii)
            core = group ^ ((xx + yy) & 1) ^ flip
            places.append(((xx * NY + yy) * NC + core) * 2 + half)
    return places


def xy_order(x, y, c, flip):
    group = c ^ ((x + y) & 1)
    own = [xy_places(x, y, group, half, flip) for half in range(2)]
    other = [xy_places(x, y, 1 - group, half, flip) for half in range(2)]
    return own[0] + own[1] + other[0][:8] + other[1][:8] + other[0][8:] + other[1][8:]


XY_COUNT = 4 * NX * NY


def order_table():
    lines = [
        xy_order(x, y, c, 0) + xy_order(x, y, c, z & 1) + z_order(c ^ (z & 1), z)
        for (x, y, c, z) in EVERY
    ]
    return np.array(lines, dtype=np.int32)


def vmem():
    return pl.BlockSpec(memory_space=pltpu.VMEM)


def smem():
    return pl.BlockSpec(memory_space=pltpu.SMEM)


def fold_rows(values):
    rows, cols = values.shape
    return jnp.sum(values.reshape(rows // 8, 8, cols), axis=0)


def fold_lanes(values):
    total = values[:, :128]
    for k in range(128, values.shape[1], 128):
        total = total + values[:, k : k + 128]
    return total


def fold(values):
    return fold_lanes(fold_rows(values))


EXTRA = 16


def write_parts(values, out, first):
    rest = values
    for k in range(3):
        part = rest.astype(jnp.bfloat16)
        rest = rest - part.astype(jnp.float32)
        block = jnp.concatenate([part, jnp.zeros_like(part)], axis=0)
        out[first : first + EXTRA, k * 128 : (k + 1) * 128] = block
    width = out.shape[1] - 384
    out[first : first + EXTRA, 384:] = jnp.zeros((EXTRA, width), jnp.bfloat16)


def read_parts(piece, first):
    total = jnp.zeros((8, 128), jnp.float32)
    for k in range(3):
        block = piece[first : first + EXTRA, k * 128 : (k + 1) * 128]
        total = total + block.astype(jnp.float32)[:8, :]
    return total


def prepare_body(matrix, tile, top, bottom):
    half = tile.shape[0] // 2
    rounded = matrix[...].astype(jnp.bfloat16)
    tile[...] = rounded
    top[...] = rounded[:half]
    bottom[...] = rounded[half:]


def prepare(matrix):
    rows, cols = matrix.shape
    shapes = [(rows, cols), (rows // 2, cols), (rows // 2, cols)]
    return pl.pallas_call(
        prepare_body,
        out_shape=[jax.ShapeDtypeStruct(s, jnp.bfloat16) for s in shapes],
        in_specs=[vmem()],
        out_specs=[vmem()] * 3,
        name="prepare",
        compiler_params=pltpu.CompilerParams(vmem_limit_bytes=4 * 2**20),
    )(matrix)


def lay_rows(order, pieces, wide, first, rows):
    cols = pieces[0].shape[1]
    stride = pieces[0].shape[0] // 2
    spot = 2 * XY_COUNT
    for piece in pieces:
        for k in range(piece.shape[0] // stride):
            start = pl.multiple_of(order[spot] * cols, 128)
            wide[first : first + rows, pl.ds(start, cols)] = piece[k * stride : k * stride + rows, :]
            spot += 1


def multiply(wide, panel, total):
    block = 2 * total.shape[1]

    def add(k, carry):
        start = pl.multiple_of(k * block, block)
        part = jnp.dot(
            wide[:, pl.ds(start, block)],
            panel[pl.ds(start, block), :],
            preferred_element_type=jnp.float32,
        )
        total[...] += part
        return carry

    total[...] = jnp.zeros(total.shape, jnp.float32)
    lax.fori_loop(0, wide.shape[1] // block, add, 0)


def first_body(step, n_right, n_left, order, *refs):
    right = refs[:n_right]
    left = refs[n_right : n_right + n_left]
    top, bottom, panel, wide, summed = refs[n_right + n_left :]
    rows, cols = summed.shape
    half = rows // 2
    spot = step * XY_COUNT
    for piece in right:
        count = piece.shape[0] // half

        def place(k, carry, piece=piece, spot=spot):
            source = pl.multiple_of(k * half, half)
            start = pl.multiple_of(order[spot + k] * half, half)
            panel[pl.ds(start, half), :] = piece[pl.ds(source, half), :]
            return carry

        lax.fori_loop(0, count, place, 0)
        spot += count
    lay_rows(order, left, wide, 0, rows)
    multiply(wide, panel, summed)
    top[:half, :] = summed[:half, :].astype(jnp.bfloat16)
    bottom[...] = summed[half:, :].astype(jnp.bfloat16)
    if step == 0:
        block = 128

        def add(k, total):
            start = pl.multiple_of(k * block, block)
            part = panel[pl.ds(start, block), :].astype(jnp.float32)
            return total + fold_rows(part * part)

        total = jnp.zeros((8, cols), jnp.float32)
        total = lax.fori_loop(0, panel.shape[0] // block, add, total)
        write_parts(fold_lanes(total), top, half)


def first_product(step, order, right, left, rows, cols):
    full = cols * NZ
    half = rows // 2
    extra = EXTRA if step == 0 else 0
    shapes = [
        jax.ShapeDtypeStruct((half + extra, cols), jnp.bfloat16),
        jax.ShapeDtypeStruct((half, cols), jnp.bfloat16),
        jax.ShapeDtypeStruct((full, cols), jnp.bfloat16),
    ]
    return pl.pallas_call(
        functools.partial(first_body, step, len(right), len(left)),
        out_shape=shapes,
        in_specs=[smem()] + [vmem()] * (len(right) + len(left)),
        out_specs=[vmem()] * len(shapes),
        scratch_shapes=[
            pltpu.VMEM((rows, full), jnp.bfloat16),
            pltpu.VMEM((rows, cols), jnp.float32),
        ],
        name="first_product",
        compiler_params=pltpu.CompilerParams(vmem_limit_bytes=14 * 2**20),
        cost_estimate=pl.CostEstimate(
            flops=2 * rows * cols * full, bytes_accessed=2 * full * cols, transcendentals=0
        ),
    )(order, *right, *left)


def second_body(last, n_left, order, shift, panel, current, *refs):
    left = refs[:n_left]
    outs = refs[n_left:]
    if last:
        earlier, outs = outs[0], outs[1:]
    wide, summed = outs[-2], outs[-1]
    rows, cols = current.shape
    half = rows // 2
    lay_rows(order, left[: n_left // 2], wide, 0, half)
    lay_rows(order, left[n_left // 2 :], wide, half, half)
    multiply(wide, panel, summed)
    value = 1.5 * current[...].astype(jnp.float32)
    if last:
        value = value - 0.5 * summed[...]
    else:
        partial = jnp.zeros((8, 128), jnp.float32)
        for piece in left[: n_left // 2]:
            for k in range(2):
                partial = partial + read_parts(piece, k * (half + EXTRA) + half)
        squares = jnp.sum(jnp.sum(partial, axis=0, keepdims=True), axis=1, keepdims=True)
        scale = TARGET * (cols * NZ) / (squares + 1e-06)
        value = jnp.sqrt(scale) * (value - 0.5 * (scale * summed[...]))
    outs[0][...] = value
    r = lax.broadcasted_iota(jnp.int32, (rows, cols), 0)
    k = lax.broadcasted_iota(jnp.int32, (rows, cols), 1)
    diagonal = fold(jnp.where(k - r == shift[0], value, 0.0))
    power = fold(value * value)
    stats = outs[1]
    if last:
        stats[:16, :] = earlier[...]
        stats[16:24, :] = diagonal
        stats[24:, :] = power
    else:
        stats[:8, :] = diagonal
        stats[8:, :] = power
        rounded = value.astype(jnp.bfloat16)
        outs[2][...] = rounded
        outs[3][...] = rounded[: rows // 2]
        outs[4][...] = rounded[rows // 2 :]


def second_product(order, shift, panel, current, left, earlier):
    last = earlier is not None
    more = [earlier] if last else []
    rows, cols = current.shape
    full = cols * NZ
    shapes = [
        jax.ShapeDtypeStruct((rows, cols), jnp.float32),
        jax.ShapeDtypeStruct((32 if last else 16, 128), jnp.float32),
    ]
    if not last:
        shapes.append(jax.ShapeDtypeStruct((rows, cols), jnp.bfloat16))
        shapes += [jax.ShapeDtypeStruct((rows // 2, cols), jnp.bfloat16)] * 2
    return pl.pallas_call(
        functools.partial(second_body, last, len(left)),
        out_shape=shapes,
        in_specs=[smem()] * 2 + [vmem()] * (2 + len(left) + len(more)),
        out_specs=[vmem()] * len(shapes),
        scratch_shapes=[
            pltpu.VMEM((rows, full), jnp.bfloat16),
            pltpu.VMEM((rows, cols), jnp.float32),
        ],
        name="second_product",
        compiler_params=pltpu.CompilerParams(vmem_limit_bytes=14 * 2**20),
        cost_estimate=pl.CostEstimate(
            flops=2 * rows * cols * full, bytes_accessed=2 * full * cols, transcendentals=0
        ),
    )(order, shift, panel, current, *left, *more)


def in_step(*values):
    return lax.optimization_barrier(values)


def to_sibling(x, y, c, z):
    return (x, y, 1 - c, z)


def panels(tile, top, bottom):
    left = []
    right = []
    piece = tile
    for turn in range(4):
        moved = permute(piece, along_z(turn % 2))
        piece = join(piece, moved) if turn == 0 else moved
        left.append(piece)
    for half, part in enumerate((top, bottom)):
        for turn in range(4):
            moved = permute(part, along_xy(turn // 2, (turn + half) % 2))
            if turn < 3:
                part = join(part, moved)
        right += [part, moved]
    first = permute(join(right[0], right[2]), to_sibling)
    second = permute(join(right[1], right[3]), to_sibling)
    return right + [first, second], left


def row_panel(top, bottom):
    left = []
    for part in (top, bottom):
        piece = part
        for turn in range(4):
            moved = permute(piece, along_z(turn % 2))
            piece = join(piece, moved) if turn == 0 else moved
            left.append(piece)
    return left


def row_target(second, turn):
    def target(x, y, c, z):
        if second:
            return (x, PAIRS[turn](y, NY), 1 - c, z)
        return (PAIRS[turn](x, NX), y, 1 - c, z)

    return target


def totals(stats):
    stats = stats + permute(stats, to_sibling)
    for k in range(4):
        stats = stats + permute(stats, row_target(k // 2, k % 2))
    for step in (1, 2, 4):
        stats = stats + permute(stats, lambda x, y, c, z: (x, y, 1 - c, z ^ step))
    return jnp.sum(stats.reshape(2, 2, 8, 128), axis=(2, 3))


def on_device(matrix):
    rows, cols = matrix.shape
    me = lax.axis_index(AXES)
    z = lax.axis_index("z")
    moved_row = z % 2 == 1
    order = lax.dynamic_index_in_dim(jnp.asarray(order_table()), me, 0, keepdims=False)
    core = jnp.bitwise_xor(lax.axis_index("c"), z % 2)
    row_first = (lax.axis_index(("x", "y")) * NC + core) * rows
    shift = (row_first - z * cols).reshape(1)
    order, shift, matrix = in_step(order, shift, matrix)
    tile, top, bottom = prepare(matrix)

    tile = jnp.where(moved_row, permute(tile, to_sibling), tile)
    right, left = panels(tile, top, bottom)
    s_top, s_bottom, panel = first_product(0, order, right, left, rows, cols)
    left = row_panel(s_top, s_bottom)
    current, stats, tile, top, bottom = second_product(order, shift, panel, tile, left, None)
    right, left = panels(tile, top, bottom)
    s_top, s_bottom, panel = first_product(1, order, right, left, rows, cols)
    left = row_panel(s_top, s_bottom)
    current, stats = second_product(order, shift, panel, current, left, stats)
    current = jnp.where(moved_row, permute(current, to_sibling), current)
    sums = totals(stats)
    return (current, sums[:, 0], jnp.sqrt(sums[:, 1]))


def solution(mesh):
    split = Mesh(mesh.devices.reshape(NX, NY, NC, NZ), AXES)
    return jax.shard_map(
        on_device,
        mesh=split,
        in_specs=(P(("x", "y", "c"), "z"),),
        out_specs=(P(("x", "y", "c"), "z"), P(), P()),
        check_vma=False,
    )
```

```python
import functools
import jax
import jax.numpy as jnp
import numpy as np
from jax import lax
from jax.experimental import pallas as pl
from jax.experimental.pallas import tpu as pltpu
from jax.sharding import Mesh
from jax.sharding import PartitionSpec as P

NX, NY, NC, NZ = 4, 4, 2, 8
AXES = ("x", "y", "c", "z")
TARGET = 0.0625

EVERY = [
    (x, y, c, z) for x in range(NX) for y in range(NY) for c in range(NC) for z in range(NZ)
]


def rank(x, y, c, z):
    return ((x * NY + y) * NC + c) * NZ + z


def even_pair(i, n):
    return i ^ 1


def odd_pair(i, n):
    return (((i - 1) % n ^ 1) + 1) % n


PAIRS = (even_pair, odd_pair)


def permute(value, target):
    return lax.ppermute(value, AXES, [(rank(*d), rank(*target(*d))) for d in EVERY])


def along_z(turn):
    return lambda x, y, c, z: (x, y, 1 - c, PAIRS[turn ^ c ^ (z & 1)](z, NZ))


def along_xy(second, turn):
    def target(x, y, c, z):
        if second ^ c ^ ((x + y) & 1):
            return (x, PAIRS[turn](y, NY), 1 - c, z)
        return (PAIRS[turn](x, NX), y, 1 - c, z)

    return target


def join(*parts):
    return jnp.concatenate(parts, axis=0)


def z_order(group, z):
    a, b = PAIRS[group], PAIRS[1 - group]
    two = lambda i: [i, a(i, NZ)]
    third = b(a(z, NZ), NZ)
    fourth = b(a(b(z, NZ), NZ), NZ)
    return two(z) + two(b(z, NZ)) + two(third) + two(fourth)


def xy_places(x, y, group, half, flip):
    a, b = PAIRS[half], PAIRS[1 - half]
    i, j = (x, y) if group == 0 else (y, x)
    four = lambda k: [k, a(k, 4), b(k, 4), a(b(k, 4), 4)]
    places = []
    for jj in four(j):
        for ii in four(i):
            xx, yy = (ii, jj) if group == 0 else (jj, ii)
            core = group ^ ((xx + yy) & 1) ^ flip
            places.append(((xx * NY + yy) * NC + core) * 2 + half)
    return places


def xy_order(x, y, c, flip):
    group = c ^ ((x + y) & 1)
    own = [xy_places(x, y, group, half, flip) for half in range(2)]
    other = [xy_places(x, y, 1 - group, half, flip) for half in range(2)]
    return own[0] + own[1] + other[0][:8] + other[1][:8] + other[0][8:] + other[1][8:]


XY_COUNT = 4 * NX * NY


def order_table():
    lines = [
        xy_order(x, y, c, 0) + xy_order(x, y, c, z & 1) + z_order(c ^ (z & 1), z)
        for (x, y, c, z) in EVERY
    ]
    return np.array(lines, dtype=np.int32)


def vmem():
    return pl.BlockSpec(memory_space=pltpu.VMEM)


def smem():
    return pl.BlockSpec(memory_space=pltpu.SMEM)


def fold_rows(values):
    rows, cols = values.shape
    return jnp.sum(values.reshape(rows // 8, 8, cols), axis=0)


def fold_lanes(values):
    total = values[:, :128]
    for k in range(128, values.shape[1], 128):
        total = total + values[:, k : k + 128]
    return total


def fold(values):
    return fold_lanes(fold_rows(values))


EXTRA = 16


def write_parts(values, out, first):
    rest = values
    for k in range(3):
        part = rest.astype(jnp.bfloat16)
        rest = rest - part.astype(jnp.float32)
        block = jnp.concatenate([part, jnp.zeros_like(part)], axis=0)
        out[first : first + EXTRA, k * 128 : (k + 1) * 128] = block
    width = out.shape[1] - 384
    out[first : first + EXTRA, 384:] = jnp.zeros((EXTRA, width), jnp.bfloat16)


def read_parts(piece, first):
    total = jnp.zeros((8, 128), jnp.float32)
    for k in range(3):
        block = piece[first : first + EXTRA, k * 128 : (k + 1) * 128]
        total = total + block.astype(jnp.float32)[:8, :]
    return total


def prepare_body(matrix, tile, top, bottom):
    half = tile.shape[0] // 2
    rounded = matrix[...].astype(jnp.bfloat16)
    tile[...] = rounded
    top[...] = rounded[:half]
    bottom[...] = rounded[half:]


def prepare(matrix):
    rows, cols = matrix.shape
    shapes = [(rows, cols), (rows // 2, cols), (rows // 2, cols)]
    return pl.pallas_call(
        prepare_body,
        out_shape=[jax.ShapeDtypeStruct(s, jnp.bfloat16) for s in shapes],
        in_specs=[vmem()],
        out_specs=[vmem()] * 3,
        name="prepare",
        compiler_params=pltpu.CompilerParams(vmem_limit_bytes=4 * 2**20),
    )(matrix)


def lay_rows(order, pieces, wide, first, rows):
    cols = pieces[0].shape[1]
    stride = pieces[0].shape[0] // 2
    spot = 2 * XY_COUNT
    for piece in pieces:
        for k in range(piece.shape[0] // stride):
            start = pl.multiple_of(order[spot] * cols, 128)
            wide[first : first + rows, pl.ds(start, cols)] = piece[k * stride : k * stride + rows, :]
            spot += 1


def multiply(wide, panel, total):
    block = 2 * total.shape[1]

    def add(k, carry):
        start = pl.multiple_of(k * block, block)
        part = jnp.dot(
            wide[:, pl.ds(start, block)],
            panel[pl.ds(start, block), :],
            preferred_element_type=jnp.float32,
        )
        total[...] += part
        return carry

    total[...] = jnp.zeros(total.shape, jnp.float32)
    lax.fori_loop(0, wide.shape[1] // block, add, 0)


def first_body(step, n_right, n_left, order, *refs):
    right = refs[:n_right]
    left = refs[n_right : n_right + n_left]
    top, bottom, panel, wide, summed = refs[n_right + n_left :]
    rows, cols = summed.shape
    half = rows // 2
    spot = step * XY_COUNT
    for piece in right:
        count = piece.shape[0] // half

        def place(k, carry, piece=piece, spot=spot):
            source = pl.multiple_of(k * half, half)
            start = pl.multiple_of(order[spot + k] * half, half)
            panel[pl.ds(start, half), :] = piece[pl.ds(source, half), :]
            return carry

        lax.fori_loop(0, count, place, 0)
        spot += count
    lay_rows(order, left, wide, 0, rows)
    multiply(wide, panel, summed)
    top[:half, :] = summed[:half, :].astype(jnp.bfloat16)
    bottom[...] = summed[half:, :].astype(jnp.bfloat16)
    if step == 0:
        block = 128

        def add(k, total):
            start = pl.multiple_of(k * block, block)
            part = panel[pl.ds(start, block), :].astype(jnp.float32)
            return total + fold_rows(part * part)

        total = jnp.zeros((8, cols), jnp.float32)
        total = lax.fori_loop(0, panel.shape[0] // block, add, total)
        write_parts(fold_lanes(total), top, half)


def first_product(step, order, right, left, rows, cols):
    full = cols * NZ
    half = rows // 2
    extra = EXTRA if step == 0 else 0
    shapes = [
        jax.ShapeDtypeStruct((half + extra, cols), jnp.bfloat16),
        jax.ShapeDtypeStruct((half, cols), jnp.bfloat16),
        jax.ShapeDtypeStruct((full, cols), jnp.bfloat16),
    ]
    return pl.pallas_call(
        functools.partial(first_body, step, len(right), len(left)),
        out_shape=shapes,
        in_specs=[smem()] + [vmem()] * (len(right) + len(left)),
        out_specs=[vmem()] * len(shapes),
        scratch_shapes=[
            pltpu.VMEM((rows, full), jnp.bfloat16),
            pltpu.VMEM((rows, cols), jnp.float32),
        ],
        name="first_product",
        compiler_params=pltpu.CompilerParams(vmem_limit_bytes=14 * 2**20),
        cost_estimate=pl.CostEstimate(
            flops=2 * rows * cols * full, bytes_accessed=2 * full * cols, transcendentals=0
        ),
    )(order, *right, *left)


def second_body(step, part, order, shift, panel, current, *refs):
    left, refs = refs[:4], list(refs[4:])
    half, cols = refs[-1].shape
    wide, summed = refs[-2:]
    taken = 0
    if part:
        stats_top = refs[0]
        taken = 1
        if step == 0:
            scale_in = refs[1]
        else:
            stats_first = refs[1]
        above = refs[2]
        taken = 3
    outs = refs[taken:-2]
    lay_rows(order, left, wide, 0, half)
    multiply(wide, panel, summed)
    first = part * half if current.shape[0] > half else 0
    value = 1.5 * current[first : first + half, :].astype(jnp.float32)
    if step == 1:
        value = value - 0.5 * summed[...]
    else:
        if part:
            scale = scale_in[:1, :1]
        else:
            partial = jnp.zeros((8, 128), jnp.float32)
            for piece in left:
                for k in range(2):
                    partial = partial + read_parts(piece, k * (half + EXTRA) + half)
            squares = jnp.sum(jnp.sum(partial, axis=0, keepdims=True), axis=1, keepdims=True)
            scale = TARGET * (cols * NZ) / (squares + 1e-06)
            outs[3][...] = jnp.broadcast_to(scale, (8, 128))
        value = jnp.sqrt(scale) * (value - 0.5 * (scale * summed[...]))
    if step and part:
        outs[0][:half, :] = above[...]
        outs[0][half:, :] = value
    else:
        outs[0][...] = value
    r = lax.broadcasted_iota(jnp.int32, (half, cols), 0) + part * half
    k = lax.broadcasted_iota(jnp.int32, (half, cols), 1)
    diagonal = fold(jnp.where(k - r == shift[0], value, 0.0))
    power = fold(value * value)
    if part:
        diagonal = diagonal + stats_top[:8, :]
        power = power + stats_top[8:, :]
    stats = outs[1]
    base = 0
    if step and part:
        stats[:16, :] = stats_first[...]
        base = 16
    stats[base : base + 8, :] = diagonal
    stats[base + 8 : base + 16, :] = power
    if step == 0:
        rounded = value.astype(jnp.bfloat16)
        outs[2][...] = rounded
        if part:
            outs[3][:half, :] = above[...]
            outs[3][half:, :] = rounded


def second_product(step, part, order, shift, panel, current, left, more):
    half, cols = left[-1].shape[0] // 2, panel.shape[1]
    if step == 0 and part == 0:
        half -= EXTRA
    full = cols * NZ
    shapes = [
        jax.ShapeDtypeStruct((2 * half if step and part else half, cols), jnp.float32),
        jax.ShapeDtypeStruct((32 if step and part else 16, 128), jnp.float32),
    ]
    if step == 0:
        shapes.append(jax.ShapeDtypeStruct((half, cols), jnp.bfloat16))
        if part == 0:
            shapes.append(jax.ShapeDtypeStruct((8, 128), jnp.float32))
        else:
            shapes.append(jax.ShapeDtypeStruct((2 * half, cols), jnp.bfloat16))
    return pl.pallas_call(
        functools.partial(second_body, step, part),
        out_shape=shapes,
        in_specs=[smem()] * 2 + [vmem()] * (2 + len(left) + len(more)),
        out_specs=[vmem()] * len(shapes),
        scratch_shapes=[
            pltpu.VMEM((half, full), jnp.bfloat16),
            pltpu.VMEM((half, cols), jnp.float32),
        ],
        name="second_product",
        compiler_params=pltpu.CompilerParams(vmem_limit_bytes=14 * 2**20),
        cost_estimate=pl.CostEstimate(
            flops=2 * half * cols * full, bytes_accessed=2 * full * cols, transcendentals=0
        ),
    )(order, shift, panel, current, *left, *more)


def in_step(*values):
    return lax.optimization_barrier(values)


def to_sibling(x, y, c, z):
    return (x, y, 1 - c, z)


def panels(tile, top, bottom):
    left = []
    right = []
    piece = tile
    for turn in range(4):
        moved = permute(piece, along_z(turn % 2))
        piece = join(piece, moved) if turn == 0 else moved
        left.append(piece)
    for half, part in enumerate((top, bottom)):
        for turn in range(4):
            moved = permute(part, along_xy(turn // 2, (turn + half) % 2))
            if turn < 3:
                part = join(part, moved)
        right += [part, moved]
    swaps = (join(right[0], right[2]), right[1], right[3])
    right += [permute(value, to_sibling) for value in swaps]
    return right, left


def row_panel(top, bottom):
    left = []
    for part in (top, bottom):
        piece = part
        for turn in range(4):
            moved = permute(piece, along_z(turn % 2))
            piece = join(piece, moved) if turn == 0 else moved
            left.append(piece)
    return left


def row_target(second, turn):
    def target(x, y, c, z):
        if second:
            return (x, PAIRS[turn](y, NY), 1 - c, z)
        return (PAIRS[turn](x, NX), y, 1 - c, z)

    return target


def totals(stats):
    targets = [to_sibling] + [row_target(k // 2, k % 2) for k in range(4)]
    targets += [lambda x, y, c, z, step=step: (x, y, 1 - c, z ^ step) for step in (1, 2, 4)]
    for target in targets:
        stats = stats + permute(stats, target)
    return jnp.sum(stats.reshape(2, 2, 8, 128), axis=(2, 3))


def on_device(matrix):
    rows, cols = matrix.shape
    me = lax.axis_index(AXES)
    z = lax.axis_index("z")
    moved_row = z % 2 == 1
    order = lax.dynamic_index_in_dim(jnp.asarray(order_table()), me, 0, keepdims=False)
    core = jnp.bitwise_xor(lax.axis_index("c"), z % 2)
    row_first = (lax.axis_index(("x", "y")) * NC + core) * rows
    shift = (row_first - z * cols).reshape(1)
    tile, top, bottom = prepare(matrix)

    tile = jnp.where(moved_row, permute(tile, to_sibling), tile)
    order, shift, tile = in_step(order, shift, tile)
    right, left = panels(tile, top, bottom)
    s_top, s_bottom, panel = first_product(0, order, right, left, rows, cols)
    left = row_panel(s_top, s_bottom)
    cur_top, stats_top, top, scale = second_product(0, 0, order, shift, panel, tile, left[:4], [])
    cur_bottom, stats_first, bottom, tile = second_product(
        0, 1, order, shift, panel, tile, left[4:], [stats_top, scale, top]
    )
    right, left = panels(tile, top, bottom)
    s_top, s_bottom, panel = first_product(1, order, right, left, rows, cols)
    left = row_panel(s_top, s_bottom)
    above, stats_top = second_product(1, 0, order, shift, panel, cur_top, left[:4], [])
    current, stats = second_product(
        1, 1, order, shift, panel, cur_bottom, left[4:], [stats_top, stats_first, above]
    )
    other = permute(current, to_sibling)
    current = jnp.where(moved_row, other, current)
    sums = totals(stats)
    return (current, sums[:, 0], jnp.sqrt(sums[:, 1]))


def solution(mesh):
    split = Mesh(mesh.devices.reshape(NX, NY, NC, NZ), AXES)
    return jax.shard_map(
        on_device,
        mesh=split,
        in_specs=(P(("x", "y", "c"), "z"),),
        out_specs=(P(("x", "y", "c"), "z"), P(), P()),
        check_vma=False,
    )
```

```python
import functools
import jax
import jax.numpy as jnp
import numpy as np
from jax import lax
from jax.experimental import pallas as pl
from jax.experimental.pallas import tpu as pltpu
from jax.sharding import Mesh
from jax.sharding import PartitionSpec as P

NX, NY, NC, NZ = 4, 4, 2, 8
AXES = ("x", "y", "c", "z")
TARGET = 0.0625

EVERY = [
    (x, y, c, z) for x in range(NX) for y in range(NY) for c in range(NC) for z in range(NZ)
]


def rank(x, y, c, z):
    return ((x * NY + y) * NC + c) * NZ + z


def even_pair(i, n):
    return i ^ 1


def odd_pair(i, n):
    return (((i - 1) % n ^ 1) + 1) % n


PAIRS = (even_pair, odd_pair)


def permute(value, target):
    return lax.ppermute(value, AXES, [(rank(*d), rank(*target(*d))) for d in EVERY])


def along_z(turn):
    return lambda x, y, c, z: (x, y, 1 - c, PAIRS[turn ^ c ^ (z & 1)](z, NZ))


def along_xy(second, turn):
    def target(x, y, c, z):
        if second ^ c ^ ((x + y) & 1):
            return (x, PAIRS[turn](y, NY), 1 - c, z)
        return (PAIRS[turn](x, NX), y, 1 - c, z)

    return target


def join(*parts):
    return jnp.concatenate(parts, axis=0)


def z_order(group, z):
    a, b = PAIRS[group], PAIRS[1 - group]
    two = lambda i: [i, a(i, NZ)]
    third = b(a(z, NZ), NZ)
    fourth = b(a(b(z, NZ), NZ), NZ)
    return two(z) + two(b(z, NZ)) + two(third) + two(fourth)


def xy_places(x, y, group, half, flip):
    a, b = PAIRS[half], PAIRS[1 - half]
    i, j = (x, y) if group == 0 else (y, x)
    four = lambda k: [k, a(k, 4), b(k, 4), a(b(k, 4), 4)]
    places = []
    for jj in four(j):
        for ii in four(i):
            xx, yy = (ii, jj) if group == 0 else (jj, ii)
            core = group ^ ((xx + yy) & 1) ^ flip
            places.append(((xx * NY + yy) * NC + core) * 2 + half)
    return places


def xy_order(x, y, c, flip):
    group = c ^ ((x + y) & 1)
    own = [xy_places(x, y, group, half, flip) for half in range(2)]
    other = [xy_places(x, y, 1 - group, half, flip) for half in range(2)]
    return own[0] + own[1] + other[0][:8] + other[1][:8] + other[0][8:] + other[1][8:]


XY_COUNT = 4 * NX * NY


def order_table():
    lines = [
        xy_order(x, y, c, 0) + xy_order(x, y, c, z & 1) + z_order(c ^ (z & 1), z)
        for (x, y, c, z) in EVERY
    ]
    return np.array(lines, dtype=np.int32)


def vmem():
    return pl.BlockSpec(memory_space=pltpu.VMEM)


def smem():
    return pl.BlockSpec(memory_space=pltpu.SMEM)


def fold_rows(values):
    rows, cols = values.shape
    return jnp.sum(values.reshape(rows // 8, 8, cols), axis=0)


def fold_lanes(values):
    total = values[:, :128]
    for k in range(128, values.shape[1], 128):
        total = total + values[:, k : k + 128]
    return total


def fold(values):
    return fold_lanes(fold_rows(values))


EXTRA = 16


def write_parts(values, out, first):
    rest = values
    for k in range(3):
        part = rest.astype(jnp.bfloat16)
        rest = rest - part.astype(jnp.float32)
        block = jnp.concatenate([part, jnp.zeros_like(part)], axis=0)
        out[first : first + EXTRA, k * 128 : (k + 1) * 128] = block
    width = out.shape[1] - 384
    out[first : first + EXTRA, 384:] = jnp.zeros((EXTRA, width), jnp.bfloat16)


def read_parts(piece, first):
    total = jnp.zeros((8, 128), jnp.float32)
    for k in range(3):
        block = piece[first : first + EXTRA, k * 128 : (k + 1) * 128]
        total = total + block.astype(jnp.float32)[:8, :]
    return total


def prepare_body(matrix, tile, top, bottom):
    half = tile.shape[0] // 2
    rounded = matrix[...].astype(jnp.bfloat16)
    tile[...] = rounded
    top[...] = rounded[:half]
    bottom[...] = rounded[half:]


def prepare(matrix):
    rows, cols = matrix.shape
    shapes = [(rows, cols), (rows // 2, cols), (rows // 2, cols)]
    return pl.pallas_call(
        prepare_body,
        out_shape=[jax.ShapeDtypeStruct(s, jnp.bfloat16) for s in shapes],
        in_specs=[vmem()],
        out_specs=[vmem()] * 3,
        name="prepare",
        compiler_params=pltpu.CompilerParams(vmem_limit_bytes=4 * 2**20),
    )(matrix)


def lay_rows(order, pieces, wide, first, rows):
    cols = pieces[0].shape[1]
    stride = pieces[0].shape[0] // 2
    spot = 2 * XY_COUNT
    for piece in pieces:
        for k in range(piece.shape[0] // stride):
            start = pl.multiple_of(order[spot] * cols, 128)
            wide[first : first + rows, pl.ds(start, cols)] = piece[k * stride : k * stride + rows, :]
            spot += 1


def multiply(wide, panel, total):
    block = 2 * total.shape[1]

    def add(k, carry):
        start = pl.multiple_of(k * block, block)
        part = jnp.dot(
            wide[:, pl.ds(start, block)],
            panel[pl.ds(start, block), :],
            preferred_element_type=jnp.float32,
        )
        total[...] += part
        return carry

    total[...] = jnp.zeros(total.shape, jnp.float32)
    lax.fori_loop(0, wide.shape[1] // block, add, 0)


def place_pieces(order, step, pieces, spots, panel, half):
    for piece, spot in zip(pieces, spots):
        base = step * XY_COUNT + spot

        def place(k, carry, piece=piece, base=base):
            source = pl.multiple_of(k * half, half)
            start = pl.multiple_of(order[base + k] * half, half)
            panel[pl.ds(start, half), :] = piece[pl.ds(source, half), :]
            return carry

        lax.fori_loop(0, piece.shape[0] // half, place, 0)


EARLY = (0, 2, 4)
EARLY_SPOTS = (0, 16, 32)
LATE = (1, 3, 5, 6)
LATE_SPOTS = (8, 24, 48, 56)


def place_body(step, half, order, *refs):
    place_pieces(order, step, refs[:-1], EARLY_SPOTS, refs[-1], half)


def place_early(step, order, pieces, half, full):
    cols = pieces[0].shape[1]
    return pl.pallas_call(
        functools.partial(place_body, step, half),
        out_shape=jax.ShapeDtypeStruct((full, cols), jnp.bfloat16),
        in_specs=[smem()] + [vmem()] * len(pieces),
        out_specs=vmem(),
        name="place_early",
        compiler_params=pltpu.CompilerParams(vmem_limit_bytes=14 * 2**20),
        cost_estimate=pl.CostEstimate(
            flops=2**28, bytes_accessed=full * cols, transcendentals=0
        ),
    )(order, *pieces)


def first_body(step, n_right, n_left, order, *refs):
    right = refs[:n_right]
    left = refs[n_right : n_right + n_left]
    top, bottom, panel, wide, summed = refs[n_right + n_left + 1 :]
    rows, cols = summed.shape
    half = rows // 2
    place_pieces(order, step, right, LATE_SPOTS, panel, half)
    lay_rows(order, left, wide, 0, rows)
    multiply(wide, panel, summed)
    top[:half, :] = summed[:half, :].astype(jnp.bfloat16)
    bottom[...] = summed[half:, :].astype(jnp.bfloat16)
    if step == 0:
        block = 128

        def add(k, total):
            start = pl.multiple_of(k * block, block)
            part = panel[pl.ds(start, block), :].astype(jnp.float32)
            return total + fold_rows(part * part)

        total = jnp.zeros((8, cols), jnp.float32)
        total = lax.fori_loop(0, panel.shape[0] // block, add, total)
        write_parts(fold_lanes(total), top, half)


def first_product(step, order, right, left, rows, cols):
    full = cols * NZ
    half = rows // 2
    extra = EXTRA if step == 0 else 0
    shapes = [
        jax.ShapeDtypeStruct((half + extra, cols), jnp.bfloat16),
        jax.ShapeDtypeStruct((half, cols), jnp.bfloat16),
        jax.ShapeDtypeStruct((full, cols), jnp.bfloat16),
    ]
    started = place_early(step, order, [right[k] for k in EARLY], half, full)
    right = [right[k] for k in LATE]
    return pl.pallas_call(
        functools.partial(first_body, step, len(right), len(left)),
        out_shape=shapes,
        in_specs=[smem()] + [vmem()] * (len(right) + len(left) + 1),
        input_output_aliases={1 + len(right) + len(left): 2},
        out_specs=[vmem()] * len(shapes),
        scratch_shapes=[
            pltpu.VMEM((rows, full), jnp.bfloat16),
            pltpu.VMEM((rows, cols), jnp.float32),
        ],
        name="first_product",
        compiler_params=pltpu.CompilerParams(vmem_limit_bytes=14 * 2**20),
        cost_estimate=pl.CostEstimate(
            flops=2 * rows * cols * full, bytes_accessed=2 * full * cols, transcendentals=0
        ),
    )(order, *right, *left, started)


def second_body(step, part, order, shift, panel, current, *refs):
    left, refs = refs[:4], list(refs[4:])
    half, cols = refs[-1].shape
    wide, summed = refs[-2:]
    taken = 0
    if part:
        stats_top = refs[0]
        taken = 1
        if step == 0:
            scale_in = refs[1]
        else:
            stats_first = refs[1]
        above = refs[2]
        taken = 3
    outs = refs[taken:-2]
    lay_rows(order, left, wide, 0, half)
    multiply(wide, panel, summed)
    first = part * half if current.shape[0] > half else 0
    value = 1.5 * current[first : first + half, :].astype(jnp.float32)
    if step == 1:
        value = value - 0.5 * summed[...]
    else:
        if part:
            scale = scale_in[:1, :1]
        else:
            partial = jnp.zeros((8, 128), jnp.float32)
            for piece in left:
                for k in range(2):
                    partial = partial + read_parts(piece, k * (half + EXTRA) + half)
            squares = jnp.sum(jnp.sum(partial, axis=0, keepdims=True), axis=1, keepdims=True)
            scale = TARGET * (cols * NZ) / (squares + 1e-06)
            outs[3][...] = jnp.broadcast_to(scale, (8, 128))
        value = jnp.sqrt(scale) * (value - 0.5 * (scale * summed[...]))
    if step and part:
        outs[0][:half, :] = above[...]
        outs[0][half:, :] = value
    else:
        outs[0][...] = value
    r = lax.broadcasted_iota(jnp.int32, (half, cols), 0) + part * half
    k = lax.broadcasted_iota(jnp.int32, (half, cols), 1)
    diagonal = fold(jnp.where(k - r == shift[0], value, 0.0))
    power = fold(value * value)
    if part:
        diagonal = diagonal + stats_top[:8, :]
        power = power + stats_top[8:, :]
    stats = outs[1]
    base = 0
    if step and part:
        stats[:16, :] = stats_first[...]
        base = 16
    stats[base : base + 8, :] = diagonal
    stats[base + 8 : base + 16, :] = power
    if step == 0:
        rounded = value.astype(jnp.bfloat16)
        outs[2][...] = rounded
        if part:
            outs[3][:half, :] = above[...]
            outs[3][half:, :] = rounded


def second_product(step, part, order, shift, panel, current, left, more):
    half, cols = left[-1].shape[0] // 2, panel.shape[1]
    if step == 0 and part == 0:
        half -= EXTRA
    full = cols * NZ
    shapes = [
        jax.ShapeDtypeStruct((2 * half if step and part else half, cols), jnp.float32),
        jax.ShapeDtypeStruct((32 if step and part else 16, 128), jnp.float32),
    ]
    if step == 0:
        shapes.append(jax.ShapeDtypeStruct((half, cols), jnp.bfloat16))
        if part == 0:
            shapes.append(jax.ShapeDtypeStruct((8, 128), jnp.float32))
        else:
            shapes.append(jax.ShapeDtypeStruct((2 * half, cols), jnp.bfloat16))
    return pl.pallas_call(
        functools.partial(second_body, step, part),
        out_shape=shapes,
        in_specs=[smem()] * 2 + [vmem()] * (2 + len(left) + len(more)),
        out_specs=[vmem()] * len(shapes),
        scratch_shapes=[
            pltpu.VMEM((half, full), jnp.bfloat16),
            pltpu.VMEM((half, cols), jnp.float32),
        ],
        name="second_product",
        compiler_params=pltpu.CompilerParams(vmem_limit_bytes=14 * 2**20),
        cost_estimate=pl.CostEstimate(
            flops=2 * half * cols * full, bytes_accessed=2 * full * cols, transcendentals=0
        ),
    )(order, shift, panel, current, *left, *more)


def in_step(*values):
    return lax.optimization_barrier(values)


def to_sibling(x, y, c, z):
    return (x, y, 1 - c, z)


def panels(tile, top, bottom):
    left = []
    right = []
    piece = tile
    for turn in range(4):
        moved = permute(piece, along_z(turn % 2))
        piece = join(piece, moved) if turn == 0 else moved
        left.append(piece)
    for half, part in enumerate((top, bottom)):
        for turn in range(4):
            moved = permute(part, along_xy(turn // 2, (turn + half) % 2))
            if turn < 3:
                part = join(part, moved)
        right += [part, moved]
    swaps = (join(right[0], right[2]), right[1], right[3])
    right += [permute(value, to_sibling) for value in swaps]
    return right, left


def row_panel(top, bottom):
    left = []
    for part in (top, bottom):
        piece = part
        for turn in range(4):
            moved = permute(piece, along_z(turn % 2))
            piece = join(piece, moved) if turn == 0 else moved
            left.append(piece)
    return left


def row_target(second, turn):
    def target(x, y, c, z):
        if second:
            return (x, PAIRS[turn](y, NY), 1 - c, z)
        return (PAIRS[turn](x, NX), y, 1 - c, z)

    return target


def totals(stats):
    targets = [to_sibling] + [row_target(k // 2, k % 2) for k in range(4)]
    targets += [lambda x, y, c, z, step=step: (x, y, 1 - c, z ^ step) for step in (1, 2, 4)]
    for target in targets:
        stats = stats + permute(stats, target)
    return jnp.sum(stats.reshape(2, 2, 8, 128), axis=(2, 3))


def on_device(matrix):
    rows, cols = matrix.shape
    me = lax.axis_index(AXES)
    z = lax.axis_index("z")
    moved_row = z % 2 == 1
    order = lax.dynamic_index_in_dim(jnp.asarray(order_table()), me, 0, keepdims=False)
    core = jnp.bitwise_xor(lax.axis_index("c"), z % 2)
    row_first = (lax.axis_index(("x", "y")) * NC + core) * rows
    shift = (row_first - z * cols).reshape(1)
    tile, top, bottom = prepare(matrix)

    tile = jnp.where(moved_row, permute(tile, to_sibling), tile)
    order, shift, tile = in_step(order, shift, tile)
    right, left = panels(tile, top, bottom)
    s_top, s_bottom, panel = first_product(0, order, right, left, rows, cols)
    left = row_panel(s_top, s_bottom)
    cur_top, stats_top, top, scale = second_product(0, 0, order, shift, panel, tile, left[:4], [])
    cur_bottom, stats_first, bottom, tile = second_product(
        0, 1, order, shift, panel, tile, left[4:], [stats_top, scale, top]
    )
    right, left = panels(tile, top, bottom)
    s_top, s_bottom, panel = first_product(1, order, right, left, rows, cols)
    left = row_panel(s_top, s_bottom)
    above, stats_top = second_product(1, 0, order, shift, panel, cur_top, left[:4], [])
    current, stats = second_product(
        1, 1, order, shift, panel, cur_bottom, left[4:], [stats_top, stats_first, above]
    )
    other = permute(current, to_sibling)
    current = jnp.where(moved_row, other, current)
    sums = totals(stats)
    return (current, sums[:, 0], jnp.sqrt(sums[:, 1]))


def solution(mesh):
    split = Mesh(mesh.devices.reshape(NX, NY, NC, NZ), AXES)
    return jax.shard_map(
        on_device,
        mesh=split,
        in_specs=(P(("x", "y", "c"), "z"),),
        out_specs=(P(("x", "y", "c"), "z"), P(), P()),
        check_vma=False,
    )
```

```python
import functools
import jax
import jax.numpy as jnp
import numpy as np
from jax import lax
from jax.experimental import pallas as pl
from jax.experimental.pallas import tpu as pltpu
from jax.sharding import Mesh
from jax.sharding import PartitionSpec as P

NX, NY, NC, NZ = 4, 4, 2, 8
AXES = ("x", "y", "c", "z")
TARGET = 0.0625

EVERY = [
    (x, y, c, z) for x in range(NX) for y in range(NY) for c in range(NC) for z in range(NZ)
]


def rank(x, y, c, z):
    return ((x * NY + y) * NC + c) * NZ + z


def even_pair(i, n):
    return i ^ 1


def odd_pair(i, n):
    return (((i - 1) % n ^ 1) + 1) % n


PAIRS = (even_pair, odd_pair)


def permute(value, target):
    return lax.ppermute(value, AXES, [(rank(*d), rank(*target(*d))) for d in EVERY])


def along_z(turn):
    return lambda x, y, c, z: (x, y, 1 - c, PAIRS[turn ^ c ^ (z & 1)](z, NZ))


def along_xy(second, turn):
    def target(x, y, c, z):
        if second ^ c ^ ((x + y) & 1):
            return (x, PAIRS[turn](y, NY), 1 - c, z)
        return (PAIRS[turn](x, NX), y, 1 - c, z)

    return target


def join(*parts):
    return jnp.concatenate(parts, axis=0)


def z_order(group, z):
    a, b = PAIRS[group], PAIRS[1 - group]
    two = lambda i: [i, a(i, NZ)]
    third = b(a(z, NZ), NZ)
    fourth = b(a(b(z, NZ), NZ), NZ)
    return two(z) + two(b(z, NZ)) + two(third) + two(fourth)


def xy_places(x, y, group, half, flip):
    a, b = PAIRS[half], PAIRS[1 - half]
    i, j = (x, y) if group == 0 else (y, x)
    four = lambda k: [k, a(k, 4), b(k, 4), a(b(k, 4), 4)]
    places = []
    for jj in four(j):
        for ii in four(i):
            xx, yy = (ii, jj) if group == 0 else (jj, ii)
            core = group ^ ((xx + yy) & 1) ^ flip
            places.append(((xx * NY + yy) * NC + core) * 2 + half)
    return places


def xy_order(x, y, c, flip):
    group = c ^ ((x + y) & 1)
    own = [xy_places(x, y, group, half, flip) for half in range(2)]
    other = [xy_places(x, y, 1 - group, half, flip) for half in range(2)]
    return own[0] + own[1] + other[0][:8] + other[1][:8] + other[0][8:] + other[1][8:]


XY_COUNT = 4 * NX * NY


def order_table():
    lines = [
        xy_order(x, y, c, 0) + xy_order(x, y, c, z & 1) + z_order(c ^ (z & 1), z)
        for (x, y, c, z) in EVERY
    ]
    return np.array(lines, dtype=np.int32)


def vmem():
    return pl.BlockSpec(memory_space=pltpu.VMEM)


def smem():
    return pl.BlockSpec(memory_space=pltpu.SMEM)


def fold_rows(values):
    rows, cols = values.shape
    return jnp.sum(values.reshape(rows // 8, 8, cols), axis=0)


def fold_lanes(values):
    total = values[:, :128]
    for k in range(128, values.shape[1], 128):
        total = total + values[:, k : k + 128]
    return total


def fold(values):
    return fold_lanes(fold_rows(values))


EXTRA = 16


def write_parts(values, out, first):
    rest = values
    for k in range(3):
        part = rest.astype(jnp.bfloat16)
        rest = rest - part.astype(jnp.float32)
        block = jnp.concatenate([part, jnp.zeros_like(part)], axis=0)
        out[first : first + EXTRA, k * 128 : (k + 1) * 128] = block
    width = out.shape[1] - 384
    out[first : first + EXTRA, 384:] = jnp.zeros((EXTRA, width), jnp.bfloat16)


def read_parts(piece, first):
    total = jnp.zeros((8, 128), jnp.float32)
    for k in range(3):
        block = piece[first : first + EXTRA, k * 128 : (k + 1) * 128]
        total = total + block.astype(jnp.float32)[:8, :]
    return total


def prepare_body(matrix, tile, top, bottom):
    half = tile.shape[0] // 2
    rounded = matrix[...].astype(jnp.bfloat16)
    tile[...] = rounded
    top[...] = rounded[:half]
    bottom[...] = rounded[half:]


def prepare(matrix):
    rows, cols = matrix.shape
    shapes = [(rows, cols), (rows // 2, cols), (rows // 2, cols)]
    return pl.pallas_call(
        prepare_body,
        out_shape=[jax.ShapeDtypeStruct(s, jnp.bfloat16) for s in shapes],
        in_specs=[vmem()],
        out_specs=[vmem()] * 3,
        name="prepare",
        compiler_params=pltpu.CompilerParams(vmem_limit_bytes=4 * 2**20),
    )(matrix)


def lay_rows(order, pieces, wide, first, rows):
    cols = pieces[0].shape[1]
    stride = pieces[0].shape[0] // 2
    spot = 2 * XY_COUNT
    for piece in pieces:
        for k in range(piece.shape[0] // stride):
            start = pl.multiple_of(order[spot] * cols, 128)
            wide[first : first + rows, pl.ds(start, cols)] = piece[k * stride : k * stride + rows, :]
            spot += 1


def multiply(wide, panel, total):
    block = 2 * total.shape[1]

    def add(k, carry):
        start = pl.multiple_of(k * block, block)
        part = jnp.dot(
            wide[:, pl.ds(start, block)],
            panel[pl.ds(start, block), :],
            preferred_element_type=jnp.float32,
        )
        total[...] += part
        return carry

    total[...] = jnp.zeros(total.shape, jnp.float32)
    lax.fori_loop(0, wide.shape[1] // block, add, 0)


def place_pieces(order, step, pieces, spots, panel, half):
    total = jnp.zeros((8, panel.shape[1]), jnp.float32)
    for piece, spot in zip(pieces, spots):
        base = step * XY_COUNT + spot

        def place(k, carry, piece=piece, base=base):
            source = pl.multiple_of(k * half, half)
            start = pl.multiple_of(order[base + k] * half, half)
            part = piece[pl.ds(source, half), :]
            panel[pl.ds(start, half), :] = part
            if step:
                return carry
            part = part.astype(jnp.float32)
            return carry + fold_rows(part * part)

        if step:
            lax.fori_loop(0, piece.shape[0] // half, place, 0)
        else:
            total = lax.fori_loop(0, piece.shape[0] // half, place, total)
    return total


EARLY = (0, 2, 4)
EARLY_SPOTS = (0, 16, 32)
LATE = (1, 3, 5, 6)
LATE_SPOTS = (8, 24, 48, 56)


def place_body(step, half, order, *refs):
    total = place_pieces(order, step, refs[:-2], EARLY_SPOTS, refs[-2], half)
    refs[-1][...] = total


def place_early(step, order, pieces, half, full):
    cols = pieces[0].shape[1]
    return pl.pallas_call(
        functools.partial(place_body, step, half),
        out_shape=[
            jax.ShapeDtypeStruct((full, cols), jnp.bfloat16),
            jax.ShapeDtypeStruct((8, cols), jnp.float32),
        ],
        in_specs=[smem()] + [vmem()] * len(pieces),
        out_specs=[vmem()] * 2,
        name="place_early",
        compiler_params=pltpu.CompilerParams(vmem_limit_bytes=14 * 2**20),
        cost_estimate=pl.CostEstimate(
            flops=2**28, bytes_accessed=full * cols, transcendentals=0
        ),
    )(order, *pieces)


def first_body(step, n_right, n_left, order, *refs):
    right = refs[:n_right]
    left = refs[n_right : n_right + n_left]
    top, bottom, panel, wide, summed = refs[n_right + n_left + 2 :]
    earlier = refs[n_right + n_left + 1]
    rows, _ = summed.shape
    half = rows // 2
    total = place_pieces(order, step, right, LATE_SPOTS, panel, half)
    lay_rows(order, left, wide, 0, rows)
    multiply(wide, panel, summed)
    top[:half, :] = summed[:half, :].astype(jnp.bfloat16)
    bottom[...] = summed[half:, :].astype(jnp.bfloat16)
    if step == 0:
        write_parts(fold_lanes(total + earlier[...]), top, half)


def first_product(step, order, right, left, rows, cols):
    full = cols * NZ
    half = rows // 2
    extra = EXTRA if step == 0 else 0
    shapes = [
        jax.ShapeDtypeStruct((half + extra, cols), jnp.bfloat16),
        jax.ShapeDtypeStruct((half, cols), jnp.bfloat16),
        jax.ShapeDtypeStruct((full, cols), jnp.bfloat16),
    ]
    started, total = place_early(step, order, [right[k] for k in EARLY], half, full)
    right = [right[k] for k in LATE]
    return pl.pallas_call(
        functools.partial(first_body, step, len(right), len(left)),
        out_shape=shapes,
        in_specs=[smem()] + [vmem()] * (len(right) + len(left) + 2),
        input_output_aliases={1 + len(right) + len(left): 2},
        out_specs=[vmem()] * len(shapes),
        scratch_shapes=[
            pltpu.VMEM((rows, full), jnp.bfloat16),
            pltpu.VMEM((rows, cols), jnp.float32),
        ],
        name="first_product",
        compiler_params=pltpu.CompilerParams(vmem_limit_bytes=14 * 2**20),
        cost_estimate=pl.CostEstimate(
            flops=2 * rows * cols * full, bytes_accessed=2 * full * cols, transcendentals=0
        ),
    )(order, *right, *left, started, total)


def second_body(step, part, order, shift, panel, current, *refs):
    left, refs = refs[:4], list(refs[4:])
    half, cols = refs[-1].shape
    wide, summed = refs[-2:]
    taken = 0
    if part:
        stats_top = refs[0]
        taken = 1
        if step == 0:
            scale_in = refs[1]
        else:
            stats_first = refs[1]
        above = refs[2]
        taken = 3
    outs = refs[taken:-2]
    lay_rows(order, left, wide, 0, half)
    multiply(wide, panel, summed)
    first = part * half if current.shape[0] > half else 0
    value = 1.5 * current[first : first + half, :].astype(jnp.float32)
    if step == 1:
        value = value - 0.5 * summed[...]
    else:
        if part:
            scale = scale_in[:1, :1]
        else:
            partial = jnp.zeros((8, 128), jnp.float32)
            for piece in left:
                for k in range(2):
                    partial = partial + read_parts(piece, k * (half + EXTRA) + half)
            squares = jnp.sum(jnp.sum(partial, axis=0, keepdims=True), axis=1, keepdims=True)
            scale = TARGET * (cols * NZ) / (squares + 1e-06)
            outs[3][...] = jnp.broadcast_to(scale, (8, 128))
        value = jnp.sqrt(scale) * (value - 0.5 * (scale * summed[...]))
    if step and part:
        outs[0][:half, :] = above[...]
        outs[0][half:, :] = value
    else:
        outs[0][...] = value
    r = lax.broadcasted_iota(jnp.int32, (half, cols), 0) + part * half
    k = lax.broadcasted_iota(jnp.int32, (half, cols), 1)
    diagonal = fold(jnp.where(k - r == shift[0], value, 0.0))
    power = fold(value * value)
    if part:
        diagonal = diagonal + stats_top[:8, :]
        power = power + stats_top[8:, :]
    stats = outs[1]
    base = 0
    if step and part:
        stats[:16, :] = stats_first[...]
        base = 16
    stats[base : base + 8, :] = diagonal
    stats[base + 8 : base + 16, :] = power
    if step == 0:
        rounded = value.astype(jnp.bfloat16)
        outs[2][...] = rounded
        if part:
            outs[3][:half, :] = above[...]
            outs[3][half:, :] = rounded


def second_product(step, part, order, shift, panel, current, left, more):
    half, cols = left[-1].shape[0] // 2, panel.shape[1]
    if step == 0 and part == 0:
        half -= EXTRA
    full = cols * NZ
    shapes = [
        jax.ShapeDtypeStruct((2 * half if step and part else half, cols), jnp.float32),
        jax.ShapeDtypeStruct((32 if step and part else 16, 128), jnp.float32),
    ]
    if step == 0:
        shapes.append(jax.ShapeDtypeStruct((half, cols), jnp.bfloat16))
        if part == 0:
            shapes.append(jax.ShapeDtypeStruct((8, 128), jnp.float32))
        else:
            shapes.append(jax.ShapeDtypeStruct((2 * half, cols), jnp.bfloat16))
    return pl.pallas_call(
        functools.partial(second_body, step, part),
        out_shape=shapes,
        in_specs=[smem()] * 2 + [vmem()] * (2 + len(left) + len(more)),
        out_specs=[vmem()] * len(shapes),
        scratch_shapes=[
            pltpu.VMEM((half, full), jnp.bfloat16),
            pltpu.VMEM((half, cols), jnp.float32),
        ],
        name="second_product",
        compiler_params=pltpu.CompilerParams(vmem_limit_bytes=14 * 2**20),
        cost_estimate=pl.CostEstimate(
            flops=2 * half * cols * full, bytes_accessed=2 * full * cols, transcendentals=0
        ),
    )(order, shift, panel, current, *left, *more)


def in_step(*values):
    return lax.optimization_barrier(values)


def to_sibling(x, y, c, z):
    return (x, y, 1 - c, z)


def panels(tile, top, bottom):
    left = []
    right = []
    piece = tile
    for turn in range(4):
        moved = permute(piece, along_z(turn % 2))
        piece = join(piece, moved) if turn == 0 else moved
        left.append(piece)
    for half, part in enumerate((top, bottom)):
        for turn in range(4):
            moved = permute(part, along_xy(turn // 2, (turn + half) % 2))
            if turn < 3:
                part = join(part, moved)
        right += [part, moved]
    swaps = (join(right[0], right[2]), right[1], right[3])
    right += [permute(value, to_sibling) for value in swaps]
    return right, left


def row_panel(top, bottom):
    left = []
    for part in (top, bottom):
        piece = part
        for turn in range(4):
            moved = permute(piece, along_z(turn % 2))
            piece = join(piece, moved) if turn == 0 else moved
            left.append(piece)
    return left


def row_target(second, turn):
    def target(x, y, c, z):
        if second:
            return (x, PAIRS[turn](y, NY), 1 - c, z)
        return (PAIRS[turn](x, NX), y, 1 - c, z)

    return target


def totals(stats):
    targets = [to_sibling] + [row_target(k // 2, k % 2) for k in range(4)]
    targets += [lambda x, y, c, z, step=step: (x, y, 1 - c, z ^ step) for step in (1, 2, 4)]
    for target in targets:
        stats = stats + permute(stats, target)
    return jnp.sum(stats.reshape(2, 2, 8, 128), axis=(2, 3))


def on_device(matrix):
    rows, cols = matrix.shape
    me = lax.axis_index(AXES)
    z = lax.axis_index("z")
    moved_row = z % 2 == 1
    order = lax.dynamic_index_in_dim(jnp.asarray(order_table()), me, 0, keepdims=False)
    core = jnp.bitwise_xor(lax.axis_index("c"), z % 2)
    row_first = (lax.axis_index(("x", "y")) * NC + core) * rows
    shift = (row_first - z * cols).reshape(1)
    tile, top, bottom = prepare(matrix)

    tile = jnp.where(moved_row, permute(tile, to_sibling), tile)
    order, shift, tile = in_step(order, shift, tile)
    right, left = panels(tile, top, bottom)
    s_top, s_bottom, panel = first_product(0, order, right, left, rows, cols)
    left = row_panel(s_top, s_bottom)
    cur_top, stats_top, top, scale = second_product(0, 0, order, shift, panel, tile, left[:4], [])
    cur_bottom, stats_first, bottom, tile = second_product(
        0, 1, order, shift, panel, tile, left[4:], [stats_top, scale, top]
    )
    right, left = panels(tile, top, bottom)
    s_top, s_bottom, panel = first_product(1, order, right, left, rows, cols)
    left = row_panel(s_top, s_bottom)
    above, stats_top = second_product(1, 0, order, shift, panel, cur_top, left[:4], [])
    current, stats = second_product(
        1, 1, order, shift, panel, cur_bottom, left[4:], [stats_top, stats_first, above]
    )
    other = permute(current, to_sibling)
    current = jnp.where(moved_row, other, current)
    sums = totals(stats)
    return (current, sums[:, 0], jnp.sqrt(sums[:, 1]))


def solution(mesh):
    split = Mesh(mesh.devices.reshape(NX, NY, NC, NZ), AXES)
    return jax.shard_map(
        on_device,
        mesh=split,
        in_specs=(P(("x", "y", "c"), "z"),),
        out_specs=(P(("x", "y", "c"), "z"), P(), P()),
        check_vma=False,
    )
```
